32 devices in a mesh: blk: 8 (over z, x), dp: 4 (over y, core).
Axes of the slice: x: 2, y: 2, z: 4, core: 2. Of those that a mesh axis runs over, the one named last changes fastest.
Arguments:
- tokens: bfloat16 [1024, 5120], P('blk', 'dp'), may hold values from -6 to 6
- expert_ids: int32 [1024, 6], P('blk'), may hold values from 0 to 15, all different within a row; in each aligned block of 128 rows (0 to 127, 128 to 255, ...) at most 96 rows name the same one
- gate_vals: float32 [1024, 6], P('blk'), may hold values from 0.1 to 1
- w_gate: bfloat16 [16, 5120, 1536], P('blk', 'dp'), may hold values from -0.078125 to 0.078125
- w_up: bfloat16 [16, 5120, 1536], P('blk', 'dp'), may hold values from -0.078125 to 0.078125
- w_down: bfloat16 [16, 5120, 1536], P('blk', 'dp'), may hold values from -0.15625 to 0.15625
Outputs:
- combined: bfloat16 [1024, 5120], P('blk', 'dp')
The draws below stay inside these ranges and needn't reach their ends.
Inputs may be any that keep to these rules, and one draw needn't show every extreme that they name: `expert_ids`: each row names 6 different experts. Among the 128 rows of one index of blk (aligned blocks) no expert is named more than 96 times, a bound that some block reaches.
All inputs are finite; a program needn't handle non-finite values.
Results may differ from the reference program's by a relative error of at most 0.0057.
Values may be sent and summed in bfloat16 or wider, within the bound.
A program may use at most 128 MiB of HBM per device.

```python
import math
import jax
import jax.numpy as jnp
import numpy as np
from jax import lax

D = 5120
FF = 1536
TOP = 6
TOK_DEV = 128
EXPERTS = 16
TOKENS = 1024
CAP = 96
N_BLK = 8


def levels(rng, shape, shards, low, top_value):
    factor_of = 1.0
    for dim, parts in shards:
        steps = jax.random.uniform(jax.random.fold_in(jax.random.fold_in(rng, 6), dim), (parts,), jnp.float32, low / len(shards), top_value / len(shards))
        factor_of = factor_of * jnp.repeat(jnp.exp(steps), shape[dim] // parts).reshape((-1,) + (1,) * (len(shape) - 1 - dim))
    return factor_of


def deal_out(rng, own, number, rows, count, top, bound, slope):
    ranking = jax.random.permutation(rng, count)
    packed, ordinary = load_shares(count, rows * top, bound, slope, True), load_shares(count, rows * top, bound, slope, False)
    places = jnp.arange(count)

    def named(tallies, turn):
        used = int((tallies > 0).sum())
        fixed = max(1, used // 4)
        moved = fixed + (places - fixed + turn * (used - fixed)) % max(1, count - fixed)
        return jnp.zeros((count,), jnp.int32).at[ranking[jnp.where(places < fixed, places, moved)]].set(jnp.asarray(tallies, jnp.int32))

    tallies = jnp.where(number % 4 == 0, named(packed, number // 4), named(ordinary, number - number // 4 - 1))
    mixed = jax.random.permutation(jax.random.fold_in(own, 3), count)
    source_of, taker = mixed[0:count // 2 * 2:2], mixed[1:count // 2 * 2:2]
    room = jnp.minimum(tallies[source_of] - 1, bound - tallies[taker]) // 2
    room = jnp.where((source_of == ranking[0]) | (taker == ranking[0]) | (tallies[taker] == 0), 0, jnp.maximum(room, 0))
    moved = jax.random.randint(jax.random.fold_in(own, 4), (count // 2,), 0, 1 << 20) % (room + 1)
    tallies = tallies.at[source_of].add(-moved).at[taker].add(moved)
    items = jnp.searchsorted(jnp.cumsum(tallies), jnp.arange(rows * top), side="right").astype(jnp.int32)
    grid = items.reshape(top, rows).T
    grid = grid[jax.random.permutation(jax.random.fold_in(own, 1), rows)]
    turn = jax.random.randint(jax.random.fold_in(own, 2), (rows, 1), 0, top)
    return jnp.take_along_axis(grid, (jnp.arange(top)[None, :] + turn) % top, axis=1)


def load_shares(amount, total, most, slope, full):
    loads = [(1 << 20) // math.isqrt(rank ** slope) + 1 for rank in range(1, amount + 1)]
    largest = most if full else min(most, max(-(-total // amount), total * loads[0] // sum(loads)))
    least = 1 if total - largest >= amount - 1 else 0
    counts, spare = [largest] + [least] * (amount - 1), total - largest - least * (amount - 1)
    while spare > 0:
        free = [i for i in range(1, amount) if counts[i] < largest] or [i for i in range(1, amount) if counts[i] < most]
        pool, remaining = sum([loads[i] for i in free]), spare
        for i in free:
            more = min(most - counts[i], max(1, remaining * loads[i] // pool), spare)
            counts[i] = counts[i] + more
            spare = spare - more
    return np.array(counts)


def gaussian(key, extent, deviation, most, split=(), held_as=jnp.bfloat16):
    array = jax.random.normal(key, extent, jnp.float32) * deviation
    if len(split) > 0:
        array = levels(key, extent, split, -0.22, 0.18) * array
    return jnp.clip(array, min=-most, max=most).astype(held_as)


def setup_inputs(seed: int = 0) -> dict:
    streams_of = jax.random.split(jax.random.key(seed), 7)
    tokens = gaussian(streams_of[0], (TOKENS, D), 1.0, 6.0, ((0, 8), (1, 4)))
    expert_ids_keys = jax.random.split(jax.random.fold_in(streams_of[1], 1), TOKENS // TOK_DEV)
    expert_ids_turns = jax.random.permutation(jax.random.fold_in(streams_of[1], 3), TOKENS // TOK_DEV)
    expert_ids = jax.vmap(lambda own, number: deal_out(jax.random.fold_in(streams_of[1], 2), own, number, TOK_DEV, EXPERTS, TOP, CAP, 2))(expert_ids_keys, expert_ids_turns).reshape((TOKENS, TOP))
    gate_vals = jnp.clip(jnp.exp(math.log(1.0) - 2.3025851 * jax.random.uniform(streams_of[2], (TOKENS, TOP), jnp.float32) ** levels(streams_of[2], (TOKENS, TOP), ((0, 8),), -0.2, 0.2)), 0.1, 1.0)
    w_gate = gaussian(streams_of[3], (EXPERTS, D, FF), D ** -0.5, 0.078125, ((0, 8), (1, 4)))
    w_up = gaussian(streams_of[4], (EXPERTS, D, FF), D ** -0.5, 0.078125, ((0, 8), (1, 4)))
    w_down = gaussian(streams_of[5], (EXPERTS, D, FF), FF ** -0.5, 0.15625, ((0, 8), (1, 4)))
    return dict(tokens=tokens, expert_ids=expert_ids, gate_vals=gate_vals, w_gate=w_gate, w_up=w_up, w_down=w_down)


def reference(tokens, expert_ids, gate_vals, w_gate, w_up, w_down):
    rows_all = N_BLK * CAP
    pairs = expert_ids.reshape(N_BLK, TOK_DEV * TOP)
    onehot = (pairs[:, :, None] == jnp.arange(EXPERTS, dtype=jnp.int32)[None, None, :]).astype(jnp.int32)
    before = jnp.cumsum(onehot, axis=1) - onehot
    position = jnp.sum(before * onehot, axis=2).astype(jnp.int32)
    source = jnp.arange(N_BLK, dtype=jnp.int32)[:, None]
    slot_index = (pairs * rows_all + source * CAP + position).reshape(-1).astype(jnp.int32)
    copies = jnp.repeat(tokens, TOP, axis=0)
    buffer = jnp.zeros((EXPERTS * rows_all, D), tokens.dtype).at[slot_index].set(copies)
    buffer = buffer.reshape(EXPERTS, rows_all, D)

    def expert_fn(items):
        row_block, gate_w, up_w, down_w = items
        gate_part = jnp.dot(row_block, gate_w, preferred_element_type=jnp.float32)
        up_part = jnp.dot(row_block, up_w, preferred_element_type=jnp.float32)
        hidden = (jax.nn.silu(gate_part) * up_part).astype(jnp.bfloat16)
        output = lax.dot_general(hidden, down_w, (((1,), (1,)), ((), ())), preferred_element_type=jnp.float32)
        return output.astype(jnp.bfloat16)

    outputs = lax.map(expert_fn, (buffer, w_gate, w_up, w_down)).reshape(EXPERTS * rows_all, D)
    picked = outputs[slot_index].astype(jnp.float32).reshape(TOKENS, TOP, D)
    combined = jnp.sum(picked * gate_vals[:, :, None], axis=1)
    return combined.astype(jnp.bfloat16)
```

```python
import jax
import jax.numpy as jnp
from jax import lax
from jax.sharding import PartitionSpec as P


def routing(expert_ids, gate_vals, held_count, capacity):
    first = lax.axis_index("blk") * held_count
    ids = lax.all_gather(expert_ids, "blk", axis=0, tiled=False)
    gates = lax.all_gather(gate_vals, "blk", axis=0, tiled=False)
    mine = first + jnp.arange(held_count, dtype=jnp.int32)
    match = ids[:, None, :, :] == mine[None, :, None, None]
    member = jnp.any(match, axis=3)
    weight = jnp.sum(jnp.where(match, gates[:, None], 0.0), axis=3)
    tok_rows = ids.shape[1]
    earlier = jnp.triu(jnp.ones((tok_rows, tok_rows), jnp.float32), 1)
    position = jnp.einsum(
        "bht,tu->bhu", member.astype(jnp.bfloat16), earlier.astype(jnp.bfloat16),
        preferred_element_type=jnp.float32,
    )
    slots = jnp.arange(capacity, dtype=jnp.int32).astype(jnp.float32)
    hot = member[:, :, None, :] & (position[:, :, None, :] == slots[None, None, :, None])
    return hot.astype(jnp.bfloat16), jnp.where(hot, weight[:, :, None, :], 0.0)


def local(tokens, expert_ids, gate_vals, w_gate, w_up, w_down):
    blk_size = lax.axis_size("blk")
    tok_rows, width_dev = tokens.shape
    top_k = expert_ids.shape[1]
    held_count = w_gate.shape[0]
    capacity = 2 * tok_rows * top_k // (held_count * blk_size)
    hot, weighted = routing(expert_ids, gate_vals, held_count, capacity)
    everyone = lax.all_gather(tokens, "blk", axis=0, tiled=False)
    routed = jnp.einsum("bhpt,btd->hbpd", hot, everyone, preferred_element_type=jnp.float32)
    routed = routed.astype(jnp.bfloat16).reshape(held_count, blk_size * capacity, width_dev)
    gate_part = jnp.einsum("emd,edf->emf", routed, w_gate, preferred_element_type=jnp.float32)
    up_part = jnp.einsum("emd,edf->emf", routed, w_up, preferred_element_type=jnp.float32)
    both = jnp.stack((gate_part, up_part), axis=0)
    summed = lax.psum_scatter(both, "dp", scatter_dimension=2, tiled=True)
    hidden = (jax.nn.silu(summed[0]) * summed[1]).astype(jnp.bfloat16)
    hidden = lax.all_gather(hidden, "dp", axis=1, tiled=True)
    result = jnp.einsum("emf,edf->emd", hidden, w_down, preferred_element_type=jnp.float32)
    result = result.astype(jnp.bfloat16).reshape(held_count, blk_size, capacity, width_dev)
    high = weighted.astype(jnp.bfloat16)
    low = (weighted - high.astype(jnp.float32)).astype(jnp.bfloat16)
    partial = jnp.einsum(
        "bhpt,hbpd->btd", high, result, preferred_element_type=jnp.float32
    ) + jnp.einsum("bhpt,hbpd->btd", low, result, preferred_element_type=jnp.float32)
    partial = partial.astype(jnp.bfloat16).reshape(blk_size * tok_rows, width_dev)
    return lax.psum_scatter(partial, "blk", scatter_dimension=0, tiled=True)


def solution(mesh):
    return jax.shard_map(
        local,
        mesh=mesh,
        in_specs=(
            P("blk", "dp"),
            P("blk", None),
            P("blk", None),
            P("blk", "dp", None),
            P("blk", "dp", None),
            P("blk", "dp", None),
        ),
        out_specs=P("blk", "dp"),
        check_vma=False,
    )
```

```python
import functools

import jax
import jax.numpy as jnp
from jax import lax
from jax.experimental import pallas as pl
from jax.experimental.pallas import tpu as pltpu
from jax.sharding import PartitionSpec as P

MESH = pl.DeviceIdType.MESH
VMEM_BYTES = 66_000_000


def flip(a, m, size):
    total, unit = 0, 1
    while unit < size:
        total = total + lax.rem(lax.div(a, unit) + lax.div(m, unit), 2) * unit
        unit *= 2
    return total


def fused_kernel(
    n_blk, tok_ref, hot_ref, high_ref, low_ref, wg_hbm, wu_hbm, wd_hbm, out_ref,
    wg, wu, wd, everyone, routed, part, near, far_out, far_in, hidden, rows_out,
    outgoing, arrived, acc,
    w_sem, tok_s, tok_r, near_s, near_r, far_s, far_r, hy_s, hy_r, hc_s, hc_r, hf_s, hf_r, ret_s, ret_r,
):
    blk = lax.axis_index("blk")
    dp = lax.axis_index("dp")
    y, c = lax.div(dp, 2), lax.rem(dp, 2)
    mate = (blk, y * 2 + (1 - c))
    across = (blk, (1 - y) * 2 + c)
    ff = wg.shape[2]
    width = wg.shape[1]
    half = part.shape[3]
    cap = 2 * half

    def copy(src, dst, send, recv, device):
        return pltpu.make_async_remote_copy(
            src_ref=src, dst_ref=dst, send_sem=send, recv_sem=recv,
            device_id=device, device_id_type=MESH,
        )

    def peer(m):
        return (flip(blk, m, n_blk), dp)

    def mask_of(i):
        m = jnp.where(i == 0, 0, jnp.where(i == 1, 2, i + 2))
        return jnp.where(i == n_blk - 2, 3, jnp.where(i == n_blk - 1, 1, m))

    def tok_direct(m):
        return copy(tok_ref, everyone.at[m], tok_s.at[m], tok_r.at[m], peer(m))

    def tok_onward(m):
        return copy(everyone.at[m], everyone.at[m + 1], tok_s.at[m + 1], tok_r.at[m + 1], peer(1))

    def near_copy(j):
        return copy(part.at[lax.rem(j, 2), 1 - c], near.at[j], near_s.at[j], near_r.at[j], mate)

    def far_copy(j):
        return copy(far_out.at[j], far_in.at[j], far_s.at[j], far_r.at[j], across)

    def hidden_far(j):
        return copy(hidden.at[j, y, c], hidden.at[j, y, c], hy_s.at[j], hy_r.at[j], across)

    def hidden_near(j):
        return copy(hidden.at[j, y, c], hidden.at[j, y, c], hc_s.at[j], hc_r.at[j], mate)

    def hidden_onward(j):
        return copy(hidden.at[j, 1 - y, c], hidden.at[j, 1 - y, c], hf_s.at[j], hf_r.at[j], mate)

    def ret_copy(m):
        return copy(outgoing.at[m], arrived.at[m], ret_s.at[m], ret_r.at[m], peer(m))

    loads = [
        pltpu.make_async_copy(wg_hbm, wg, w_sem.at[0]),
        pltpu.make_async_copy(wu_hbm, wu, w_sem.at[1]),
        pltpu.make_async_copy(wd_hbm, wd, w_sem.at[2]),
    ]
    for load in loads:
        load.start()

    barrier = pltpu.get_barrier_semaphore()
    for m in range(1, n_blk):
        pl.semaphore_signal(barrier, inc=1, device_id=peer(m), device_id_type=MESH)
    for device in (mate, across):
        pl.semaphore_signal(barrier, inc=1, device_id=device, device_id_type=MESH)
    pl.semaphore_wait(barrier, n_blk + 1)

    for m in [1] + list(range(2, n_blk, 2)):
        tok_direct(m).start()
    everyone[0] = tok_ref[...]

    def project(i):
        m = mask_of(i)

        @pl.when(i > 0)
        def _():
            tok_direct(m).wait_recv()

        @pl.when((m > 0) & (lax.rem(m, 2) == 0))
        def _():
            tok_onward(m).start()

        routed[...] = jnp.dot(
            hot_ref[flip(blk, m, n_blk)], everyone[m], preferred_element_type=jnp.float32
        ).astype(jnp.bfloat16)

        @pl.when(i == 0)
        def _():
            loads[0].wait()
            loads[1].wait()

        slot = lax.rem(i, 2)
        tile = ff // 3 if ff % 384 == 0 else ff
        for h in range(2):
            rows = routed[h * cap:(h + 1) * cap, :]
            for which, w in enumerate((wg, wu)):
                for f in range(0, ff, tile):
                    got = jnp.dot(rows, w[h, :, f:f + tile], preferred_element_type=jnp.float32)
                    at = which * ff + f
                    part[slot, 0, h, :, at:at + tile] = got[:half]
                    part[slot, 1, h, :, at:at + tile] = got[half:]
        near_copy(i).start()

    def join(j):
        near_copy(j).wait()
        slot = lax.rem(j, 2)
        far_out[j] = (part[slot, c, 1 - y] + near[j, 1 - y]).astype(jnp.bfloat16)
        far_copy(j).start()
        near[j, y] = near[j, y] + part[slot, c, y]

    def activate(j):
        far_copy(j).wait_recv()
        gate = near[j, y, :, :ff] + far_in[j, :, :ff].astype(jnp.float32)
        up = near[j, y, :, ff:] + far_in[j, :, ff:].astype(jnp.float32)
        hidden[j, y, c] = (gate / (1.0 + jnp.exp(-gate)) * up).astype(jnp.bfloat16)
        hidden_far(j).start()
        hidden_near(j).start()

    def relay(j):
        hidden_far(j).wait_recv()
        hidden_onward(j).start()

    def finish(j):
        @pl.when(j == 0)
        def _():
            loads[2].wait()

        hidden_near(j).wait_recv()
        hidden_onward(j).wait_recv()
        m = mask_of(j)
        tile = 256 if width % 256 == 0 else width
        for h in range(2):
            rows = hidden[j, h].reshape(cap, ff)
            for d in range(0, width, tile):
                rows_out[h * cap:(h + 1) * cap, d:d + tile] = lax.dot_general(
                    rows, wd[h, d:d + tile, :], (((1,), (1,)), ((), ())),
                    preferred_element_type=jnp.float32,
                ).astype(jnp.bfloat16)
        target = flip(blk, m, n_blk)
        mixed = jnp.dot(high_ref[target], rows_out[...], preferred_element_type=jnp.float32)
        mixed = mixed + jnp.dot(low_ref[target], rows_out[...], preferred_element_type=jnp.float32)

        @pl.when(m == 0)
        def _():
            acc[...] = mixed

        @pl.when(m > 0)
        def _():
            outgoing[m] = mixed.astype(jnp.bfloat16)
            ret_copy(m).start()

    stages = (project, join, activate, relay, finish)

    def step(i, carry):
        for lag, stage in enumerate(stages):
            @pl.when((i >= lag) & (i - lag < n_blk))
            def _():
                stage(i - lag)
        return carry

    lax.fori_loop(0, n_blk + len(stages) - 1, step, 0)

    def gather_in(m, carry):
        ret_copy(m).wait_recv()
        acc[...] += arrived[m].astype(jnp.float32)
        return carry

    lax.fori_loop(1, n_blk, gather_in, 0)
    out_ref[...] = acc[...].astype(jnp.bfloat16)

    def drain(m, carry):
        far_copy(m).wait_send()
        hidden_far(m).wait_send()
        hidden_near(m).wait_send()
        hidden_onward(m).wait_send()

        @pl.when(m > 0)
        def _():
            tok_direct(m).wait_send()
            ret_copy(m).wait_send()

        return carry

    lax.fori_loop(0, n_blk, drain, 0)


def fused(tokens, expert_ids, gate_vals, w_gate, w_up, w_down):
    n_blk = lax.axis_size("blk")
    tok_rows, width = tokens.shape
    held, _, ff = w_gate.shape
    capacity = 2 * tok_rows * expert_ids.shape[1] // (held * n_blk)
    slots, half = held * capacity, capacity // 2
    hot, weighted = routing(expert_ids, gate_vals, held, capacity)
    hot = hot.reshape(n_blk, slots, tok_rows)
    weighted = weighted.reshape(n_blk, slots, tok_rows).transpose(0, 2, 1)
    high = weighted.astype(jnp.bfloat16)
    low = (weighted - high.astype(jnp.float32)).astype(jnp.bfloat16)
    bf, f32 = jnp.bfloat16, jnp.float32
    sems = [pltpu.SemaphoreType.DMA((n_blk,)) for _ in range(14)]
    vmem = pl.BlockSpec(memory_space=pltpu.VMEM)
    anywhere = pl.BlockSpec(memory_space=pl.ANY)
    return pl.pallas_call(
        functools.partial(fused_kernel, n_blk),
        out_shape=jax.ShapeDtypeStruct((tok_rows, width), bf),
        in_specs=[vmem] * 4 + [anywhere] * 3,
        out_specs=vmem,
        scratch_shapes=[
            pltpu.VMEM(w_gate.shape, bf),
            pltpu.VMEM(w_up.shape, bf),
            pltpu.VMEM(w_down.shape, bf),
            pltpu.VMEM((n_blk, tok_rows, width), bf),
            pltpu.VMEM((slots, width), bf),
            pltpu.VMEM((2, 2, held, half, 2 * ff), f32),
            pltpu.VMEM((n_blk, held, half, 2 * ff), f32),
            pltpu.VMEM((n_blk, half, 2 * ff), bf),
            pltpu.VMEM((n_blk, half, 2 * ff), bf),
            pltpu.VMEM((n_blk, held, 2, half, ff), bf),
            pltpu.VMEM((slots, width), bf),
            pltpu.VMEM((n_blk, tok_rows, width), bf),
            pltpu.VMEM((n_blk, tok_rows, width), bf),
            pltpu.VMEM((tok_rows, width), f32),
            pltpu.SemaphoreType.DMA((3,)),
        ] + sems,
        compiler_params=pltpu.CompilerParams(
            collective_id=0, has_side_effects=True, vmem_limit_bytes=VMEM_BYTES
        ),
    )(tokens, hot, high, low, w_gate, w_up, w_down)


def routing(expert_ids, gate_vals, held_count, capacity):
    first = lax.axis_index("blk") * held_count
    top_k = expert_ids.shape[1]
    both = jnp.concatenate((expert_ids.astype(jnp.float32), gate_vals), axis=1)
    both = lax.all_gather(both, "blk", axis=0, tiled=False)
    ids, gates = both[:, :, :top_k].astype(jnp.int32), both[:, :, top_k:]
    mine = first + jnp.arange(held_count, dtype=jnp.int32)
    match = ids[:, None, :, :] == mine[None, :, None, None]
    member = jnp.any(match, axis=3)
    weight = jnp.sum(jnp.where(match, gates[:, None], 0.0), axis=3)
    tok_rows = ids.shape[1]
    earlier = jnp.triu(jnp.ones((tok_rows, tok_rows), jnp.float32), 1)
    position = jnp.einsum(
        "bht,tu->bhu", member.astype(jnp.bfloat16), earlier.astype(jnp.bfloat16),
        preferred_element_type=jnp.float32,
    )
    slots = jnp.arange(capacity, dtype=jnp.int32).astype(jnp.float32)
    hot = member[:, :, None, :] & (position[:, :, None, :] == slots[None, None, :, None])
    return hot.astype(jnp.bfloat16), jnp.where(hot, weight[:, :, None, :], 0.0)


def local(tokens, expert_ids, gate_vals, w_gate, w_up, w_down):
    blk_size = lax.axis_size("blk")
    tok_rows, width_dev = tokens.shape
    top_k = expert_ids.shape[1]
    held_count = w_gate.shape[0]
    capacity = 2 * tok_rows * top_k // (held_count * blk_size)
    hot, weighted = routing(expert_ids, gate_vals, held_count, capacity)
    everyone = lax.all_gather(tokens, "blk", axis=0, tiled=False)
    routed = jnp.einsum("bhpt,btd->hbpd", hot, everyone, preferred_element_type=jnp.float32)
    routed = routed.astype(jnp.bfloat16).reshape(held_count, blk_size * capacity, width_dev)
    gate_part = jnp.einsum("emd,edf->emf", routed, w_gate, preferred_element_type=jnp.float32)
    up_part = jnp.einsum("emd,edf->emf", routed, w_up, preferred_element_type=jnp.float32)
    both = jnp.stack((gate_part, up_part), axis=0)
    summed = lax.psum_scatter(both, "dp", scatter_dimension=2, tiled=True)
    hidden = (jax.nn.silu(summed[0]) * summed[1]).astype(jnp.bfloat16)
    hidden = lax.all_gather(hidden, "dp", axis=1, tiled=True)
    result = jnp.einsum("emf,edf->emd", hidden, w_down, preferred_element_type=jnp.float32)
    result = result.astype(jnp.bfloat16).reshape(held_count, blk_size, capacity, width_dev)
    high = weighted.astype(jnp.bfloat16)
    low = (weighted - high.astype(jnp.float32)).astype(jnp.bfloat16)
    partial = jnp.einsum(
        "bhpt,hbpd->btd", high, result, preferred_element_type=jnp.float32
    ) + jnp.einsum("bhpt,hbpd->btd", low, result, preferred_element_type=jnp.float32)
    partial = partial.astype(jnp.bfloat16).reshape(blk_size * tok_rows, width_dev)
    return lax.psum_scatter(partial, "blk", scatter_dimension=0, tiled=True)


def choose(tokens, expert_ids, gate_vals, w_gate, w_up, w_down):
    n_blk, held = lax.axis_size("blk"), w_gate.shape[0]
    capacity = 2 * tokens.shape[0] * expert_ids.shape[1] // (held * n_blk)
    fits = lax.axis_size("dp") == 4 and held == 2 and n_blk == 8 and capacity % 32 == 0
    body = fused if fits else local
    return body(tokens, expert_ids, gate_vals, w_gate, w_up, w_down)


def solution(mesh):
    return jax.shard_map(
        choose,
        mesh=mesh,
        in_specs=(
            P("blk", "dp"),
            P("blk", None),
            P("blk", None),
            P("blk", "dp", None),
            P("blk", "dp", None),
            P("blk", "dp", None),
        ),
        out_specs=P("blk", "dp"),
        check_vma=False,
    )
```

```python
import functools

import jax
import jax.numpy as jnp
from jax import lax
from jax.experimental import pallas as pl
from jax.experimental.pallas import tpu as pltpu
from jax.sharding import PartitionSpec as P

MESH = pl.DeviceIdType.MESH
VMEM_BYTES = 66_000_000


def flip(a, m, size):
    total, unit = 0, 1
    while unit < size:
        total = total + lax.rem(lax.div(a, unit) + lax.div(m, unit), 2) * unit
        unit *= 2
    return total


def fused_kernel(
    n_blk, tok_ref, info_ref, wg_hbm, wu_hbm, wd_hbm, out_ref,
    wg, wu, wd, everyone, routed, part, near, far_out, far_in, hidden, rows_out,
    outgoing, arrived, acc, info, high, low, hot,
    w_sem, tok_s, tok_r, near_s, near_r, far_s, far_r, hy_s, hy_r, hc_s, hc_r, hf_s, hf_r, ret_s, ret_r, info_s, info_r,
):
    blk = lax.axis_index("blk")
    dp = lax.axis_index("dp")
    y, c = lax.div(dp, 2), lax.rem(dp, 2)
    mate = (blk, y * 2 + (1 - c))
    across = (blk, (1 - y) * 2 + c)
    ff = wg.shape[2]
    width = wg.shape[1]
    half = part.shape[3]
    cap = 2 * half

    def copy(src, dst, send, recv, device):
        return pltpu.make_async_remote_copy(
            src_ref=src, dst_ref=dst, send_sem=send, recv_sem=recv,
            device_id=device, device_id_type=MESH,
        )

    def peer(m):
        return (flip(blk, m, n_blk), dp)

    def mask_of(i):
        m = jnp.where(i == 0, 0, jnp.where(i == 1, 2, i + 2))
        return jnp.where(i == n_blk - 2, 3, jnp.where(i == n_blk - 1, 1, m))

    def tok_direct(m):
        return copy(tok_ref, everyone.at[m], tok_s.at[m], tok_r.at[m], peer(m))

    def info_direct(m):
        return copy(info_ref, info.at[m], info_s.at[m], info_r.at[m], peer(m))

    def tok_onward(m):
        return copy(everyone.at[m], everyone.at[m + 1], tok_s.at[m + 1], tok_r.at[m + 1], peer(1))

    def near_copy(j):
        return copy(part.at[lax.rem(j, 2), 1 - c], near.at[j], near_s.at[j], near_r.at[j], mate)

    def far_copy(j):
        return copy(far_out.at[j], far_in.at[j], far_s.at[j], far_r.at[j], across)

    def hidden_far(j):
        return copy(hidden.at[j, y, c], hidden.at[j, y, c], hy_s.at[j], hy_r.at[j], across)

    def hidden_near(j):
        return copy(hidden.at[j, y, c], hidden.at[j, y, c], hc_s.at[j], hc_r.at[j], mate)

    def hidden_onward(j):
        return copy(hidden.at[j, 1 - y, c], hidden.at[j, 1 - y, c], hf_s.at[j], hf_r.at[j], mate)

    def ret_copy(m):
        return copy(outgoing.at[m], arrived.at[m], ret_s.at[m], ret_r.at[m], peer(m))

    loads = [
        pltpu.make_async_copy(wg_hbm, wg, w_sem.at[0]),
        pltpu.make_async_copy(wu_hbm, wu, w_sem.at[1]),
        pltpu.make_async_copy(wd_hbm, wd, w_sem.at[2]),
    ]
    for load in loads:
        load.start()

    barrier = pltpu.get_barrier_semaphore()
    for m in range(1, n_blk):
        pl.semaphore_signal(barrier, inc=1, device_id=peer(m), device_id_type=MESH)
    for device in (mate, across):
        pl.semaphore_signal(barrier, inc=1, device_id=device, device_id_type=MESH)
    pl.semaphore_wait(barrier, n_blk + 1)

    for m in range(1, n_blk):
        info_direct(m).start()
    for m in [1] + list(range(2, n_blk, 2)):
        tok_direct(m).start()
    everyone[0] = tok_ref[...]
    info[0] = info_ref[...]
    tok_rows = tok_ref.shape[0]
    lines = info_ref.shape[0] // 2

    def slots_of(m):
        square = (tok_rows, tok_rows)
        before = lax.broadcasted_iota(jnp.int32, square, 0) < lax.broadcasted_iota(jnp.int32, square, 1)
        before = jnp.where(before, 1.0, 0.0).astype(jnp.bfloat16)
        slot = lax.broadcasted_iota(jnp.int32, (cap, tok_rows), 0).astype(jnp.float32)
        ids, gates = info[m, :lines], info[m, lines:]
        for h in range(2):
            match = ids == (2 * blk + h).astype(jnp.float32)
            member = jnp.sum(jnp.where(match, 1.0, 0.0), axis=0, keepdims=True)
            weight = jnp.sum(jnp.where(match, gates, 0.0), axis=0, keepdims=True)
            wide = jnp.broadcast_to(member, (16, tok_rows)).astype(jnp.bfloat16)
            position = jnp.dot(wide, before, preferred_element_type=jnp.float32)[0:1]
            taken = (slot == position) & (member > 0.5)
            weighted = jnp.where(taken, weight, 0.0)
            top = weighted.astype(jnp.bfloat16)
            span = slice(h * cap, (h + 1) * cap)
            high[m, span, :] = top
            low[m, span, :] = (weighted - top.astype(jnp.float32)).astype(jnp.bfloat16)
            hot[span, :] = jnp.where(taken, 1.0, 0.0).astype(jnp.bfloat16)

    def project(i):
        m = mask_of(i)

        @pl.when(i > 0)
        def _():
            info_direct(m).wait_recv()
            tok_direct(m).wait_recv()

        @pl.when((m > 0) & (lax.rem(m, 2) == 0))
        def _():
            tok_onward(m).start()

        slots_of(m)
        routed[...] = jnp.dot(
            hot[...], everyone[m], preferred_element_type=jnp.float32
        ).astype(jnp.bfloat16)

        @pl.when(i == 0)
        def _():
            loads[0].wait()
            loads[1].wait()

        slot = lax.rem(i, 2)
        tile = ff // 3 if ff % 384 == 0 else ff
        for h in range(2):
            rows = routed[h * cap:(h + 1) * cap, :]
            for which, w in enumerate((wg, wu)):
                for f in range(0, ff, tile):
                    got = jnp.dot(rows, w[h, :, f:f + tile], preferred_element_type=jnp.float32)
                    at = which * ff + f
                    part[slot, 0, h, :, at:at + tile] = got[:half]
                    part[slot, 1, h, :, at:at + tile] = got[half:]
        near_copy(i).start()

    def join(j):
        near_copy(j).wait()
        slot = lax.rem(j, 2)
        far_out[j] = (part[slot, c, 1 - y] + near[j, 1 - y]).astype(jnp.bfloat16)
        far_copy(j).start()
        near[j, y] = near[j, y] + part[slot, c, y]

    def activate(j):
        far_copy(j).wait_recv()
        gate = near[j, y, :, :ff] + far_in[j, :, :ff].astype(jnp.float32)
        up = near[j, y, :, ff:] + far_in[j, :, ff:].astype(jnp.float32)
        hidden[j, y, c] = (gate / (1.0 + jnp.exp(-gate)) * up).astype(jnp.bfloat16)
        hidden_far(j).start()
        hidden_near(j).start()

    def relay(j):
        hidden_far(j).wait_recv()
        hidden_onward(j).start()

    def finish(j):
        @pl.when(j == 0)
        def _():
            loads[2].wait()

        hidden_near(j).wait_recv()
        hidden_onward(j).wait_recv()
        m = mask_of(j)
        tile = 256 if width % 256 == 0 else width
        for h in range(2):
            rows = hidden[j, h].reshape(cap, ff)
            for d in range(0, width, tile):
                rows_out[h * cap:(h + 1) * cap, d:d + tile] = lax.dot_general(
                    rows, wd[h, d:d + tile, :], (((1,), (1,)), ((), ())),
                    preferred_element_type=jnp.float32,
                ).astype(jnp.bfloat16)
        over_slots = (((0,), (0,)), ((), ()))
        mixed = lax.dot_general(high[m], rows_out[...], over_slots, preferred_element_type=jnp.float32)
        mixed = mixed + lax.dot_general(
            low[m], rows_out[...], over_slots, preferred_element_type=jnp.float32
        )

        @pl.when(m == 0)
        def _():
            acc[...] = mixed

        @pl.when(m > 0)
        def _():
            outgoing[m] = mixed.astype(jnp.bfloat16)
            ret_copy(m).start()

    stages = ((1, join), (2, activate), (0, project), (3, relay), (4, finish))

    def step(i, carry):
        for lag, stage in stages:
            @pl.when((i >= lag) & (i - lag < n_blk))
            def _():
                stage(i - lag)
        return carry

    lax.fori_loop(0, n_blk + len(stages) - 1, step, 0)

    def gather_in(m, carry):
        ret_copy(m).wait_recv()
        acc[...] += arrived[m].astype(jnp.float32)
        return carry

    lax.fori_loop(1, n_blk, gather_in, 0)
    out_ref[...] = acc[...].astype(jnp.bfloat16)

    def drain(m, carry):
        far_copy(m).wait_send()
        hidden_far(m).wait_send()
        hidden_near(m).wait_send()
        hidden_onward(m).wait_send()

        @pl.when(m > 0)
        def _():
            info_direct(m).wait_send()
            tok_direct(m).wait_send()
            ret_copy(m).wait_send()

        return carry

    lax.fori_loop(0, n_blk, drain, 0)


def fused(tokens, expert_ids, gate_vals, w_gate, w_up, w_down):
    n_blk = lax.axis_size("blk")
    tok_rows, width = tokens.shape
    held, _, ff = w_gate.shape
    capacity = 2 * tok_rows * expert_ids.shape[1] // (held * n_blk)
    slots, half = held * capacity, capacity // 2
    top_k = expert_ids.shape[1]
    spare = ((0, -top_k % 8), (0, 0))
    ids = jnp.pad(expert_ids.T.astype(jnp.float32), spare, constant_values=-1.0)
    packed = jnp.concatenate((ids, jnp.pad(gate_vals.T, spare)), axis=0)
    bf, f32 = jnp.bfloat16, jnp.float32
    sems = [pltpu.SemaphoreType.DMA((n_blk,)) for _ in range(16)]
    vmem = pl.BlockSpec(memory_space=pltpu.VMEM)
    anywhere = pl.BlockSpec(memory_space=pl.ANY)
    return pl.pallas_call(
        functools.partial(fused_kernel, n_blk),
        out_shape=jax.ShapeDtypeStruct((tok_rows, width), bf),
        in_specs=[vmem] * 2 + [anywhere] * 3,
        out_specs=vmem,
        scratch_shapes=[
            pltpu.VMEM(w_gate.shape, bf),
            pltpu.VMEM(w_up.shape, bf),
            pltpu.VMEM(w_down.shape, bf),
            pltpu.VMEM((n_blk, tok_rows, width), bf),
            pltpu.VMEM((slots, width), bf),
            pltpu.VMEM((2, 2, held, half, 2 * ff), f32),
            pltpu.VMEM((n_blk, held, half, 2 * ff), f32),
            pltpu.VMEM((n_blk, half, 2 * ff), bf),
            pltpu.VMEM((n_blk, half, 2 * ff), bf),
            pltpu.VMEM((n_blk, held, 2, half, ff), bf),
            pltpu.VMEM((slots, width), bf),
            pltpu.VMEM((n_blk, tok_rows, width), bf),
            pltpu.VMEM((n_blk, tok_rows, width), bf),
            pltpu.VMEM((tok_rows, width), f32),
            pltpu.VMEM((n_blk,) + packed.shape, f32),
            pltpu.VMEM((n_blk, slots, tok_rows), bf),
            pltpu.VMEM((n_blk, slots, tok_rows), bf),
            pltpu.VMEM((slots, tok_rows), bf),
            pltpu.SemaphoreType.DMA((3,)),
        ] + sems,
        compiler_params=pltpu.CompilerParams(
            collective_id=0, has_side_effects=True, vmem_limit_bytes=VMEM_BYTES
        ),
    )(tokens, packed, w_gate, w_up, w_down)


def routing(expert_ids, gate_vals, held_count, capacity):
    first = lax.axis_index("blk") * held_count
    top_k = expert_ids.shape[1]
    both = jnp.concatenate((expert_ids.astype(jnp.float32), gate_vals), axis=1)
    both = lax.all_gather(both, "blk", axis=0, tiled=False)
    ids, gates = both[:, :, :top_k].astype(jnp.int32), both[:, :, top_k:]
    mine = first + jnp.arange(held_count, dtype=jnp.int32)
    match = ids[:, None, :, :] == mine[None, :, None, None]
    member = jnp.any(match, axis=3)
    weight = jnp.sum(jnp.where(match, gates[:, None], 0.0), axis=3)
    tok_rows = ids.shape[1]
    earlier = jnp.triu(jnp.ones((tok_rows, tok_rows), jnp.float32), 1)
    position = jnp.einsum(
        "bht,tu->bhu", member.astype(jnp.bfloat16), earlier.astype(jnp.bfloat16),
        preferred_element_type=jnp.float32,
    )
    slots = jnp.arange(capacity, dtype=jnp.int32).astype(jnp.float32)
    hot = member[:, :, None, :] & (position[:, :, None, :] == slots[None, None, :, None])
    return hot.astype(jnp.bfloat16), jnp.where(hot, weight[:, :, None, :], 0.0)


def local(tokens, expert_ids, gate_vals, w_gate, w_up, w_down):
    blk_size = lax.axis_size("blk")
    tok_rows, width_dev = tokens.shape
    top_k = expert_ids.shape[1]
    held_count = w_gate.shape[0]
    capacity = 2 * tok_rows * top_k // (held_count * blk_size)
    hot, weighted = routing(expert_ids, gate_vals, held_count, capacity)
    everyone = lax.all_gather(tokens, "blk", axis=0, tiled=False)
    routed = jnp.einsum("bhpt,btd->hbpd", hot, everyone, preferred_element_type=jnp.float32)
    routed = routed.astype(jnp.bfloat16).reshape(held_count, blk_size * capacity, width_dev)
    gate_part = jnp.einsum("emd,edf->emf", routed, w_gate, preferred_element_type=jnp.float32)
    up_part = jnp.einsum("emd,edf->emf", routed, w_up, preferred_element_type=jnp.float32)
    both = jnp.stack((gate_part, up_part), axis=0)
    summed = lax.psum_scatter(both, "dp", scatter_dimension=2, tiled=True)
    hidden = (jax.nn.silu(summed[0]) * summed[1]).astype(jnp.bfloat16)
    hidden = lax.all_gather(hidden, "dp", axis=1, tiled=True)
    result = jnp.einsum("emf,edf->emd", hidden, w_down, preferred_element_type=jnp.float32)
    result = result.astype(jnp.bfloat16).reshape(held_count, blk_size, capacity, width_dev)
    high = weighted.astype(jnp.bfloat16)
    low = (weighted - high.astype(jnp.float32)).astype(jnp.bfloat16)
    partial = jnp.einsum(
        "bhpt,hbpd->btd", high, result, preferred_element_type=jnp.float32
    ) + jnp.einsum("bhpt,hbpd->btd", low, result, preferred_element_type=jnp.float32)
    partial = partial.astype(jnp.bfloat16).reshape(blk_size * tok_rows, width_dev)
    return lax.psum_scatter(partial, "blk", scatter_dimension=0, tiled=True)


def choose(tokens, expert_ids, gate_vals, w_gate, w_up, w_down):
    n_blk, held = lax.axis_size("blk"), w_gate.shape[0]
    capacity = 2 * tokens.shape[0] * expert_ids.shape[1] // (held * n_blk)
    fits = lax.axis_size("dp") == 4 and held == 2 and n_blk == 8 and capacity % 32 == 0
    body = fused if fits else local
    return body(tokens, expert_ids, gate_vals, w_gate, w_up, w_down)


def solution(mesh):
    return jax.shard_map(
        choose,
        mesh=mesh,
        in_specs=(
            P("blk", "dp"),
            P("blk", None),
            P("blk", None),
            P("blk", "dp", None),
            P("blk", "dp", None),
            P("blk", "dp", None),
        ),
        out_specs=P("blk", "dp"),
        check_vma=False,
    )
```

```python
import functools

import jax
import jax.numpy as jnp
from jax import lax
from jax.experimental import pallas as pl
from jax.experimental.pallas import tpu as pltpu
from jax.sharding import PartitionSpec as P

MESH = pl.DeviceIdType.MESH
VMEM_BYTES = 66_000_000


def flip(a, m, size):
    total, unit = 0, 1
    while unit < size:
        total = total + lax.rem(lax.div(a, unit) + lax.div(m, unit), 2) * unit
        unit *= 2
    return total


def fused_kernel(
    n_blk, tok_ref, info_ref, wg_hbm, wu_hbm, wd_hbm, out_ref,
    wg, wu, wd, everyone, routed, part, near, far_out, far_in, hidden, rows_out,
    outgoing, arrived, acc, info, high, low, hot,
    w_sem, tok_s, tok_r, near_s, near_r, far_s, far_r, hy_s, hy_r, hc_s, hc_r, hf_s, hf_r, ret_s, ret_r, info_s, info_r,
):
    blk = lax.axis_index("blk")
    dp = lax.axis_index("dp")
    y, c = lax.div(dp, 2), lax.rem(dp, 2)
    mate = (blk, y * 2 + (1 - c))
    across = (blk, (1 - y) * 2 + c)
    ff = wg.shape[2]
    width = wg.shape[1]
    half = part.shape[3]
    cap = 2 * half

    def copy(src, dst, send, recv, device):
        return pltpu.make_async_remote_copy(
            src_ref=src, dst_ref=dst, send_sem=send, recv_sem=recv,
            device_id=device, device_id_type=MESH,
        )

    def peer(m):
        return (flip(blk, m, n_blk), dp)

    def mask_of(i):
        m = jnp.where(i == 0, 0, jnp.where(i == 1, 2, i + 2))
        return jnp.where(i == n_blk - 2, 3, jnp.where(i == n_blk - 1, 1, m))

    def tok_direct(m):
        return copy(tok_ref, everyone.at[m], tok_s.at[m], tok_r.at[m], peer(m))

    def info_direct(m):
        return copy(info_ref, info.at[m], info_s.at[m], info_r.at[m], peer(m))

    def tok_onward(m):
        return copy(everyone.at[m], everyone.at[m + 1], tok_s.at[m + 1], tok_r.at[m + 1], peer(1))

    def near_copy(j):
        return copy(part.at[lax.rem(j, 2), 1 - c], near.at[j], near_s.at[j], near_r.at[j], mate)

    def far_copy(j):
        return copy(far_out.at[j], far_in.at[j], far_s.at[j], far_r.at[j], across)

    def hidden_far(j):
        return copy(hidden.at[j, y, c], hidden.at[j, y, c], hy_s.at[j], hy_r.at[j], across)

    def hidden_near(j):
        return copy(hidden.at[j, y, c], hidden.at[j, y, c], hc_s.at[j], hc_r.at[j], mate)

    def hidden_onward(j):
        return copy(hidden.at[j, 1 - y, c], hidden.at[j, 1 - y, c], hf_s.at[j], hf_r.at[j], mate)

    def ret_copy(m):
        return copy(outgoing.at[m], arrived.at[m], ret_s.at[m], ret_r.at[m], peer(m))

    loads = [
        pltpu.make_async_copy(wg_hbm, wg, w_sem.at[0]),
        pltpu.make_async_copy(wu_hbm, wu, w_sem.at[1]),
        pltpu.make_async_copy(wd_hbm, wd, w_sem.at[2]),
    ]
    loads[0].start()
    loads[1].start()

    barrier = pltpu.get_barrier_semaphore()
    for m in range(1, n_blk):
        pl.semaphore_signal(barrier, inc=1, device_id=peer(m), device_id_type=MESH)
    for device in (mate, across):
        pl.semaphore_signal(barrier, inc=1, device_id=device, device_id_type=MESH)
    pl.semaphore_wait(barrier, n_blk + 1)

    for m in range(1, n_blk):
        info_direct(m).start()
    for m in [1] + list(range(2, n_blk, 2)):
        tok_direct(m).start()
    everyone[0] = tok_ref[...]
    info[0] = info_ref[...]
    tok_rows = tok_ref.shape[0]
    lines = info_ref.shape[0] // 2

    def slots_of(m):
        square = (tok_rows, tok_rows)
        before = lax.broadcasted_iota(jnp.int32, square, 0) < lax.broadcasted_iota(jnp.int32, square, 1)
        before = jnp.where(before, 1.0, 0.0).astype(jnp.bfloat16)
        slot = lax.broadcasted_iota(jnp.int32, (cap, tok_rows), 0).astype(jnp.float32)
        ids, gates = info[m, :lines], info[m, lines:]
        for h in range(2):
            match = ids == (2 * blk + h).astype(jnp.float32)
            member = jnp.sum(jnp.where(match, 1.0, 0.0), axis=0, keepdims=True)
            weight = jnp.sum(jnp.where(match, gates, 0.0), axis=0, keepdims=True)
            wide = jnp.broadcast_to(member, (16, tok_rows)).astype(jnp.bfloat16)
            position = jnp.dot(wide, before, preferred_element_type=jnp.float32)[0:1]
            taken = (slot == position) & (member > 0.5)
            weighted = jnp.where(taken, weight, 0.0)
            top = weighted.astype(jnp.bfloat16)
            span = slice(h * cap, (h + 1) * cap)
            high[m, span, :] = top
            low[m, span, :] = (weighted - top.astype(jnp.float32)).astype(jnp.bfloat16)
            hot[span, :] = jnp.where(taken, 1.0, 0.0).astype(jnp.bfloat16)

    def project(i):
        m = mask_of(i)

        @pl.when(i > 0)
        def _():
            info_direct(m).wait_recv()
            tok_direct(m).wait_recv()

        @pl.when((m > 0) & (lax.rem(m, 2) == 0))
        def _():
            tok_onward(m).start()

        slots_of(m)
        routed[...] = jnp.dot(
            hot[...], everyone[m], preferred_element_type=jnp.float32
        ).astype(jnp.bfloat16)

        slot = lax.rem(i, 2)
        tile = ff // 3 if ff % 384 == 0 else ff
        for which, w in enumerate((wg, wu)):
            @pl.when(i == 0)
            def _():
                loads[which].wait()
                if which == 1:
                    loads[2].start()

            for h in range(2):
                rows = routed[h * cap:(h + 1) * cap, :]
                for f in range(0, ff, tile):
                    got = jnp.dot(rows, w[h, :, f:f + tile], preferred_element_type=jnp.float32)
                    at = which * ff + f
                    part[slot, 0, h, :, at:at + tile] = got[:half]
                    part[slot, 1, h, :, at:at + tile] = got[half:]
        near_copy(i).start()

    def join(j):
        near_copy(j).wait()
        slot = lax.rem(j, 2)
        far_out[j] = (part[slot, c, 1 - y] + near[j, 1 - y]).astype(jnp.bfloat16)
        far_copy(j).start()
        near[j, y] = near[j, y] + part[slot, c, y]

    def activate(j):
        far_copy(j).wait_recv()
        gate = near[j, y, :, :ff] + far_in[j, :, :ff].astype(jnp.float32)
        up = near[j, y, :, ff:] + far_in[j, :, ff:].astype(jnp.float32)
        hidden[j, y, c] = (gate / (1.0 + jnp.exp(-gate)) * up).astype(jnp.bfloat16)
        hidden_far(j).start()
        hidden_near(j).start()

    def relay(j):
        hidden_far(j).wait_recv()
        hidden_onward(j).start()

    def finish(j):
        @pl.when(j == 0)
        def _():
            loads[2].wait()

        hidden_near(j).wait_recv()
        hidden_onward(j).wait_recv()
        m = mask_of(j)
        tile = 256 if width % 256 == 0 else width
        for h in range(2):
            rows = hidden[j, h].reshape(cap, ff)
            for d in range(0, width, tile):
                rows_out[h * cap:(h + 1) * cap, d:d + tile] = lax.dot_general(
                    rows, wd[h, d:d + tile, :], (((1,), (1,)), ((), ())),
                    preferred_element_type=jnp.float32,
                ).astype(jnp.bfloat16)
        over_slots = (((0,), (0,)), ((), ()))
        mixed = lax.dot_general(high[m], rows_out[...], over_slots, preferred_element_type=jnp.float32)
        mixed = mixed + lax.dot_general(
            low[m], rows_out[...], over_slots, preferred_element_type=jnp.float32
        )

        @pl.when(m == 0)
        def _():
            acc[...] = mixed

        @pl.when(m > 0)
        def _():
            outgoing[m] = mixed.astype(jnp.bfloat16)
            ret_copy(m).start()

    stages = ((1, join), (2, activate), (0, project), (3, relay), (4, finish))

    def step(i, carry):
        for lag, stage in stages:
            @pl.when((i >= lag) & (i - lag < n_blk))
            def _():
                stage(i - lag)
        return carry

    lax.fori_loop(0, n_blk + len(stages) - 1, step, 0)

    def gather_in(m, carry):
        ret_copy(m).wait_recv()
        acc[...] += arrived[m].astype(jnp.float32)
        return carry

    lax.fori_loop(1, n_blk, gather_in, 0)
    out_ref[...] = acc[...].astype(jnp.bfloat16)

    def drain(m, carry):
        far_copy(m).wait_send()
        hidden_far(m).wait_send()
        hidden_near(m).wait_send()
        hidden_onward(m).wait_send()

        @pl.when(m > 0)
        def _():
            info_direct(m).wait_send()
            tok_direct(m).wait_send()
            ret_copy(m).wait_send()

        return carry

    lax.fori_loop(0, n_blk, drain, 0)


def fused(tokens, expert_ids, gate_vals, w_gate, w_up, w_down):
    n_blk = lax.axis_size("blk")
    tok_rows, width = tokens.shape
    held, _, ff = w_gate.shape
    capacity = 2 * tok_rows * expert_ids.shape[1] // (held * n_blk)
    slots, half = held * capacity, capacity // 2
    top_k = expert_ids.shape[1]
    spare = ((0, -top_k % 8), (0, 0))
    ids = jnp.pad(expert_ids.T.astype(jnp.float32), spare, constant_values=-1.0)
    packed = jnp.concatenate((ids, jnp.pad(gate_vals.T, spare)), axis=0)
    bf, f32 = jnp.bfloat16, jnp.float32
    sems = [pltpu.SemaphoreType.DMA((n_blk,)) for _ in range(16)]
    vmem = pl.BlockSpec(memory_space=pltpu.VMEM)
    anywhere = pl.BlockSpec(memory_space=pl.ANY)
    return pl.pallas_call(
        functools.partial(fused_kernel, n_blk),
        out_shape=jax.ShapeDtypeStruct((tok_rows, width), bf),
        in_specs=[vmem] * 2 + [anywhere] * 3,
        out_specs=vmem,
        scratch_shapes=[
            pltpu.VMEM(w_gate.shape, bf),
            pltpu.VMEM(w_up.shape, bf),
            pltpu.VMEM(w_down.shape, bf),
            pltpu.VMEM((n_blk, tok_rows, width), bf),
            pltpu.VMEM((slots, width), bf),
            pltpu.VMEM((2, 2, held, half, 2 * ff), f32),
            pltpu.VMEM((n_blk, held, half, 2 * ff), f32),
            pltpu.VMEM((n_blk, half, 2 * ff), bf),
            pltpu.VMEM((n_blk, half, 2 * ff), bf),
            pltpu.VMEM((n_blk, held, 2, half, ff), bf),
            pltpu.VMEM((slots, width), bf),
            pltpu.VMEM((n_blk, tok_rows, width), bf),
            pltpu.VMEM((n_blk, tok_rows, width), bf),
            pltpu.VMEM((tok_rows, width), f32),
            pltpu.VMEM((n_blk,) + packed.shape, f32),
            pltpu.VMEM((n_blk, slots, tok_rows), bf),
            pltpu.VMEM((n_blk, slots, tok_rows), bf),
            pltpu.VMEM((slots, tok_rows), bf),
            pltpu.SemaphoreType.DMA((3,)),
        ] + sems,
        compiler_params=pltpu.CompilerParams(
            collective_id=0, has_side_effects=True, vmem_limit_bytes=VMEM_BYTES
        ),
    )(tokens, packed, w_gate, w_up, w_down)


def routing(expert_ids, gate_vals, held_count, capacity):
    first = lax.axis_index("blk") * held_count
    top_k = expert_ids.shape[1]
    both = jnp.concatenate((expert_ids.astype(jnp.float32), gate_vals), axis=1)
    both = lax.all_gather(both, "blk", axis=0, tiled=False)
    ids, gates = both[:, :, :top_k].astype(jnp.int32), both[:, :, top_k:]
    mine = first + jnp.arange(held_count, dtype=jnp.int32)
    match = ids[:, None, :, :] == mine[None, :, None, None]
    member = jnp.any(match, axis=3)
    weight = jnp.sum(jnp.where(match, gates[:, None], 0.0), axis=3)
    tok_rows = ids.shape[1]
    earlier = jnp.triu(jnp.ones((tok_rows, tok_rows), jnp.float32), 1)
    position = jnp.einsum(
        "bht,tu->bhu", member.astype(jnp.bfloat16), earlier.astype(jnp.bfloat16),
        preferred_element_type=jnp.float32,
    )
    slots = jnp.arange(capacity, dtype=jnp.int32).astype(jnp.float32)
    hot = member[:, :, None, :] & (position[:, :, None, :] == slots[None, None, :, None])
    return hot.astype(jnp.bfloat16), jnp.where(hot, weight[:, :, None, :], 0.0)


def local(tokens, expert_ids, gate_vals, w_gate, w_up, w_down):
    blk_size = lax.axis_size("blk")
    tok_rows, width_dev = tokens.shape
    top_k = expert_ids.shape[1]
    held_count = w_gate.shape[0]
    capacity = 2 * tok_rows * top_k // (held_count * blk_size)
    hot, weighted = routing(expert_ids, gate_vals, held_count, capacity)
    everyone = lax.all_gather(tokens, "blk", axis=0, tiled=False)
    routed = jnp.einsum("bhpt,btd->hbpd", hot, everyone, preferred_element_type=jnp.float32)
    routed = routed.astype(jnp.bfloat16).reshape(held_count, blk_size * capacity, width_dev)
    gate_part = jnp.einsum("emd,edf->emf", routed, w_gate, preferred_element_type=jnp.float32)
    up_part = jnp.einsum("emd,edf->emf", routed, w_up, preferred_element_type=jnp.float32)
    both = jnp.stack((gate_part, up_part), axis=0)
    summed = lax.psum_scatter(both, "dp", scatter_dimension=2, tiled=True)
    hidden = (jax.nn.silu(summed[0]) * summed[1]).astype(jnp.bfloat16)
    hidden = lax.all_gather(hidden, "dp", axis=1, tiled=True)
    result = jnp.einsum("emf,edf->emd", hidden, w_down, preferred_element_type=jnp.float32)
    result = result.astype(jnp.bfloat16).reshape(held_count, blk_size, capacity, width_dev)
    high = weighted.astype(jnp.bfloat16)
    low = (weighted - high.astype(jnp.float32)).astype(jnp.bfloat16)
    partial = jnp.einsum(
        "bhpt,hbpd->btd", high, result, preferred_element_type=jnp.float32
    ) + jnp.einsum("bhpt,hbpd->btd", low, result, preferred_element_type=jnp.float32)
    partial = partial.astype(jnp.bfloat16).reshape(blk_size * tok_rows, width_dev)
    return lax.psum_scatter(partial, "blk", scatter_dimension=0, tiled=True)


def choose(tokens, expert_ids, gate_vals, w_gate, w_up, w_down):
    n_blk, held = lax.axis_size("blk"), w_gate.shape[0]
    capacity = 2 * tokens.shape[0] * expert_ids.shape[1] // (held * n_blk)
    fits = lax.axis_size("dp") == 4 and held == 2 and n_blk == 8 and capacity % 32 == 0
    body = fused if fits else local
    return body(tokens, expert_ids, gate_vals, w_gate, w_up, w_down)


def solution(mesh):
    return jax.shard_map(
        choose,
        mesh=mesh,
        in_specs=(
            P("blk", "dp"),
            P("blk", None),
            P("blk", None),
            P("blk", "dp", None),
            P("blk", "dp", None),
            P("blk", "dp", None),
        ),
        out_specs=P("blk", "dp"),
        check_vma=False,
    )
```
